32 devices in a mesh: grp: 2 (over x), seq: 16 (over z, y, core).
Axes of the slice: x: 2, y: 2, z: 4, core: 2. Of those that a mesh axis runs over, the one named last changes fastest.
Arguments:
- queries: bfloat16 [8, 16, 8192], P('grp', 'seq'), parts along dimension 0, may hold values from -100 to 100
- answer_keys: bfloat16 [8, 16, 1024], P('grp', 'seq'), parts along dimension 0, may hold values from -6 to 6
- answer_values: bfloat16 [8, 16, 1024], P('grp', 'seq'), parts along dimension 0, may hold values from -6 to 6
- cached_prefix_keys: bfloat16 [2048, 1024], P(('grp', 'seq')), parts along dimension 0, may hold values from -5 to 5
- cached_prefix_values: bfloat16 [2048, 1024], P(('grp', 'seq')), parts along dimension 0, may hold values from -6 to 6
- residual: bfloat16 [8, 16, 8192], P('grp', 'seq'), parts along dimension 0, may hold values from -0.4375 to 0.4375
- out_weight: bfloat16 [8192, 8192], P('seq'), may hold values from -0.0625 to 0.0625
- norm_gain: float32 [8192], replicated, may hold values from 0.5 to 1.5
- head_weight: bfloat16 [8192, 65536], P(None, 'seq'), may hold values from -0.5745243 to 0.5745243
- targets: int32 [8, 16], P('grp'), parts along dimension 0, may hold values from 0 to 65535
- score_mask: int32 [8, 16], P('grp'), parts along dimension 0, may hold values 0 or 1
- lengths: int32 [8], P('grp'), parts along dimension 0, may hold values from 1 to 16, 40 in all
Outputs:
- logprobs: float32 [8, 16], P('grp', 'seq'), parts along dimension 0
- scores: float32 [8], P('grp'), parts along dimension 0
The draws below stay inside these ranges and needn't reach their ends.
There are 2 independent parts, one for each index of `grp`. The reference program is written for one: setup_inputs(seed, part) draws one part's arguments, and reference() takes and returns one part's arrays. A program takes and returns all parts, laid end to end along the dimension named above; an argument that names none is the same for every part. Nothing has to cross between parts.
All inputs are finite; a program needn't handle non-finite values.
Results may differ from the reference program's by a relative error of at most 0.0013.
Values may be sent and summed in bfloat16 or wider, within the bound.
A program may use at most 128 MiB of HBM per device.

```python
import math
from functools import partial
import jax
import jax.numpy as jnp
import numpy as np
from jax import lax

D = 8192
QUERY_HEADS = 64
KEY_VALUE_HEADS = 8
HEAD_SIZE = 128
VOCAB = 65536
CHOICE_COUNT = 4
CHOICE_LENGTH = 16
PREFIX_LENGTH = 1024


def key_lookup(key):
    sampled_draws = jax.random.truncated_normal(jax.random.fold_in(key, 7101), -4.5, 4.5, (PREFIX_LENGTH, KEY_VALUE_HEADS * HEAD_SIZE), jnp.float32)
    return sampled_draws


def draw_cached_prefix_keys(key, part):
    return key_lookup(key).astype(jnp.bfloat16)


def draw_queries(key, part):
    sampled_draws = jax.random.truncated_normal(jax.random.fold_in(key, 7105), -4.5, 4.5, (CHOICE_COUNT, CHOICE_LENGTH, QUERY_HEADS * HEAD_SIZE), jnp.float32)
    return sampled_draws.astype(jnp.bfloat16)


def draw_head_weight(key, part):
    sampled_draws = jax.random.truncated_normal(jax.random.fold_in(key, 7107), -5.0, 5.0, (D, VOCAB), jnp.float32) * (3.5 / math.sqrt(D))
    return sampled_draws.astype(jnp.bfloat16)


def plant(result, key, least, largest):
    dims = result.shape
    place = [jax.random.randint(jax.random.fold_in(key, axis), (), 0, dims[axis]) for axis in range(len(dims))]
    result = result.at[tuple(place)].set(least)
    longest = dims.index(max(dims))
    place[longest] = (place[longest] + 1) % dims[longest]
    return result.at[tuple(place)].set(largest)


def block_scale(rng, shape, shards, low, top_value):
    level, own = 1.0, jax.random.fold_in(rng, 6)
    for position, parts in shards:
        steps = jnp.exp(jax.random.uniform(jax.random.fold_in(own, position), (parts,), jnp.float32, low / len(shards), top_value / len(shards)))
        level = level * jnp.repeat(steps, shape[position] // parts).reshape([-1 if axis == position else 1 for axis in range(len(shape))])
    return level


def profile(number_of, total, most, lean):
    weights = [(1 << 20) // math.isqrt(rank ** lean) + 1 for rank in range(2, number_of + 1)]
    surplus, given = total - most - (number_of - 1), [1] * (number_of - 1)
    while surplus > 0:
        free = [i for i in range(number_of - 1) if given[i] < most]
        mass, budget = sum([weights[i] for i in free]), surplus
        for i in free:
            addition = min(most - given[i], max(1, budget * weights[i] // mass), surplus)
            given[i] = given[i] + addition
            surplus = surplus - addition
    return np.array([most] + given)


def uneven(stream_key, count, total, bound, slope):
    if count == 2:
        one = jax.random.randint(stream_key, (), max(1, total - bound), min(bound, total - 1) + 1)
        return jnp.stack([one, total - one])
    sizes = jnp.asarray(profile(count, total, bound, slope), jnp.int32)
    couples = (count - 1) // 2
    donor, receiver = sizes[1:1 + 2 * couples:2], sizes[2:2 + 2 * couples:2]
    margin = jnp.minimum(donor - 1, bound - receiver)
    shifted = jax.random.randint(jax.random.fold_in(stream_key, 1), (couples,), 0, 1 << 20) % (margin + 1)
    sizes = sizes.at[1:1 + 2 * couples:2].set(donor - shifted).at[2:2 + 2 * couples:2].set(receiver + shifted)
    return sizes[jax.random.permutation(jax.random.fold_in(stream_key, 2), count)]


def noise(rng, extent, width, limit, cuts=(), dtype=jnp.bfloat16):
    gain = block_scale(rng, extent, cuts, -0.22, 0.18) if cuts else 1.0
    drawn = jax.random.normal(rng, extent, jnp.float32) * width * gain
    return jnp.minimum(jnp.maximum(drawn, -limit), limit).astype(dtype)


def setup_inputs(seed: int = 0, part: int = 0) -> dict:
    streams_of = jax.random.split(jax.random.key(seed), 13)
    own_keys = jax.random.split(jax.random.fold_in(streams_of[12], part), 13)
    queries = draw_queries(jax.random.fold_in(jax.random.fold_in(streams_of[12], part), 71), part)
    answer_keys = noise(own_keys[1], (CHOICE_COUNT, CHOICE_LENGTH, KEY_VALUE_HEADS * HEAD_SIZE), 1.0, 6.0, ((1, 16),))
    answer_values = noise(own_keys[2], (CHOICE_COUNT, CHOICE_LENGTH, KEY_VALUE_HEADS * HEAD_SIZE), 1.0, 6.0, ((1, 16),))
    cached_prefix_keys = draw_cached_prefix_keys(jax.random.fold_in(jax.random.fold_in(streams_of[12], part), 71), part)
    cached_prefix_values = noise(own_keys[4], (PREFIX_LENGTH, KEY_VALUE_HEADS * HEAD_SIZE), 1.0, 6.0, ((0, 16),))
    residual = noise(own_keys[5], (CHOICE_COUNT, CHOICE_LENGTH, D), 0.03, 0.4375, ((1, 16),))
    out_weight = noise(streams_of[6], (QUERY_HEADS * HEAD_SIZE, D), (QUERY_HEADS * HEAD_SIZE) ** -0.5, 0.0625, ((0, 16),))
    norm_gain = jnp.clip(1.0 + 0.1 * jax.random.normal(streams_of[7], (D,), jnp.float32), 0.5, 1.5)
    head_weight = draw_head_weight(jax.random.fold_in(streams_of[12], 71), part)
    targets = plant(jax.random.randint(own_keys[9], (CHOICE_COUNT, CHOICE_LENGTH), 0, VOCAB), jax.random.fold_in(own_keys[9], 1), 0, VOCAB - 1).astype(jnp.int32)
    score_mask = plant((jax.random.randint(own_keys[10], (CHOICE_COUNT, CHOICE_LENGTH), 0, 4) < 3).astype(jnp.int32), jax.random.fold_in(own_keys[10], 1), 0, 1)
    lengths = uneven(own_keys[11], CHOICE_COUNT, 5 * CHOICE_LENGTH // 2, CHOICE_LENGTH, 2).astype(jnp.int32)
    return dict(queries=queries, answer_keys=answer_keys, answer_values=answer_values, cached_prefix_keys=cached_prefix_keys, cached_prefix_values=cached_prefix_values, residual=residual, out_weight=out_weight, norm_gain=norm_gain, head_weight=head_weight, targets=targets, score_mask=score_mask, lengths=lengths)


def choice_attention_step(operands, prefix_key_rows, prefix_value_rows):
    query_vector, answer_own_keys, answer_own_values = operands
    scaling = HEAD_SIZE ** (-0.5)
    grouped_queries = query_vector.astype(jnp.float32).reshape(CHOICE_LENGTH, KEY_VALUE_HEADS, QUERY_HEADS // KEY_VALUE_HEADS, HEAD_SIZE)
    self_keys = answer_own_keys.astype(jnp.float32).reshape(CHOICE_LENGTH, KEY_VALUE_HEADS, HEAD_SIZE)
    self_values = answer_own_values.astype(jnp.float32).reshape(CHOICE_LENGTH, KEY_VALUE_HEADS, HEAD_SIZE)
    prefix_scores = jnp.einsum('lkgd,pkd->kglp', grouped_queries, prefix_key_rows) * scaling
    choice_scores = jnp.einsum('lkgd,skd->kgls', grouped_queries, self_keys) * scaling
    causal = lax.broadcasted_iota(jnp.int32, (CHOICE_LENGTH, CHOICE_LENGTH), 0) >= lax.broadcasted_iota(jnp.int32, (CHOICE_LENGTH, CHOICE_LENGTH), 1)
    choice_scores = jnp.where(causal, choice_scores, -1e+30)
    row_peak = jnp.maximum(prefix_scores.max(-1), choice_scores.max(-1))[..., None]
    prefix_exp = jnp.exp(prefix_scores - row_peak)
    choice_exp = jnp.exp(choice_scores - row_peak)
    normalizer = prefix_exp.sum(-1, keepdims=True) + choice_exp.sum(-1, keepdims=True)
    weights_pre = (prefix_exp / normalizer).astype(jnp.bfloat16)
    choice_own_weights = (choice_exp / normalizer).astype(jnp.bfloat16)
    mixed = jnp.einsum('kglp,pkd->lkgd', weights_pre.astype(jnp.float32), prefix_value_rows)
    mixed = mixed + jnp.einsum('kgls,skd->lkgd', choice_own_weights.astype(jnp.float32), self_values)
    return mixed.astype(jnp.bfloat16).reshape(CHOICE_LENGTH, QUERY_HEADS * HEAD_SIZE)

def reference(queries, answer_keys, answer_values, cached_prefix_keys, cached_prefix_values, residual, out_weight, norm_gain, head_weight, targets, score_mask, lengths):
    prefix_key_rows = cached_prefix_keys.astype(jnp.float32).reshape(PREFIX_LENGTH, KEY_VALUE_HEADS, HEAD_SIZE)
    prefix_value_rows = cached_prefix_values.astype(jnp.float32).reshape(PREFIX_LENGTH, KEY_VALUE_HEADS, HEAD_SIZE)
    attended_output_rows = lax.map(partial(choice_attention_step, prefix_key_rows=prefix_key_rows, prefix_value_rows=prefix_value_rows), (queries, answer_keys, answer_values))
    update = jnp.dot(attended_output_rows.reshape(CHOICE_COUNT * CHOICE_LENGTH, QUERY_HEADS * HEAD_SIZE), out_weight, preferred_element_type=jnp.float32)
    hidden = residual.astype(jnp.float32) + update.reshape(CHOICE_COUNT, CHOICE_LENGTH, D)
    inv_rms = lax.rsqrt(lax.optimization_barrier(jnp.mean(hidden * hidden, -1, keepdims=True)) + 1e-05)
    normalized_hidden = (hidden * inv_rms * norm_gain).astype(jnp.bfloat16)
    logits = jnp.dot(normalized_hidden.reshape(CHOICE_COUNT * CHOICE_LENGTH, D), head_weight, preferred_element_type=jnp.float32)
    global_max = logits.max(-1)
    exp_total = lax.optimization_barrier(jnp.sum(jnp.exp(logits - global_max[:, None]), -1))
    target_logit = jnp.take_along_axis(logits, targets.reshape(CHOICE_COUNT * CHOICE_LENGTH, 1).astype(jnp.int32), axis=1)[:, 0]
    logprobs = (target_logit - global_max - jnp.log(exp_total)).reshape(CHOICE_COUNT, CHOICE_LENGTH)
    positions = lax.broadcasted_iota(jnp.int32, (CHOICE_COUNT, CHOICE_LENGTH), 1)
    usable = jnp.where((score_mask == 1) & (positions < lengths[:, None]), 1.0, 0.0).astype(jnp.float32)
    counted = jnp.maximum(lax.optimization_barrier(jnp.sum(usable, -1)), 1.0)
    scores = lax.optimization_barrier(jnp.sum(logprobs * usable, -1)) / counted
    return (logprobs, scores)
```

```python
import functools

import jax
import jax.numpy as jnp
from jax import lax
from jax.experimental import pallas as pl
from jax.experimental.pallas import tpu as pltpu
from jax.sharding import PartitionSpec as P

D = 8192
QUERY_HEADS = 64
KEY_VALUE_HEADS = 8
HEAD_SIZE = 128
CHOICE_COUNT = 4


def partner(block, axis, distance):
    count = lax.axis_size(axis)
    route = []
    for low in range(count):
        high = low | 1 << distance
        if high != low and high < count:
            route += [(low, high), (high, low)]
    return lax.ppermute(block, axis, route)


def combined_all(x, axis, combine):
    everything = jax.tree.map(lambda part: lax.all_gather(part, axis), x)
    leading = jax.tree.map(lambda part: part[0], everything)

    def hop(k, so_far):
        return combine(so_far, jax.tree.map(lambda part: part[k], everything))

    return lax.fori_loop(1, lax.axis_size(axis), hop, leading)


def per_device(
    queries,
    answer_keys,
    answer_values,
    cached_prefix_keys,
    cached_prefix_values,
    residual,
    out_weight,
    norm_gain,
    head_weight,
    targets,
    score_mask,
    lengths,
):
    seq_count = lax.axis_size("seq")
    myself = lax.axis_index("seq")
    local_length = queries.shape[1]
    full_len = local_length * seq_count
    groups = max(1, seq_count // QUERY_HEADS)
    per_dev = QUERY_HEADS * groups // seq_count
    grouped_heads = QUERY_HEADS // per_dev
    per_group = CHOICE_COUNT // groups
    repeat_count = grouped_heads // KEY_VALUE_HEADS
    local_prefix = cached_prefix_keys.shape[0]
    query_items = queries.reshape(
        groups, per_group, local_length, grouped_heads, per_dev * HEAD_SIZE
    )
    query_items = query_items.transpose(3, 0, 1, 2, 4).reshape(
        seq_count, per_group, local_length, per_dev * HEAD_SIZE
    )

    def choice_entries(input_array):
        expanded_heads = jnp.repeat(
            input_array.reshape(CHOICE_COUNT, local_length, KEY_VALUE_HEADS, HEAD_SIZE),
            repeat_count,
            axis=2,
        )
        expanded_heads = expanded_heads.reshape(
            groups, per_group, local_length, grouped_heads, HEAD_SIZE
        ).transpose(3, 0, 1, 2, 4)
        return expanded_heads.reshape(seq_count, per_group, local_length, HEAD_SIZE)

    def prefix_items(input_array):
        expanded_heads = jnp.repeat(
            input_array.reshape(local_prefix, KEY_VALUE_HEADS, HEAD_SIZE), repeat_count, axis=1
        ).transpose(1, 0, 2)
        expanded_heads = jnp.broadcast_to(
            expanded_heads[:, None, None], (grouped_heads, groups, 1, local_prefix, HEAD_SIZE)
        )
        return expanded_heads.reshape(seq_count, 1, local_prefix, HEAD_SIZE)

    head_queries, head_keys, head_values, head_pkeys, head_pvalues = (
        lax.all_to_all(query_items, "seq", split_axis=0, concat_axis=2, tiled=True),
        lax.all_to_all(choice_entries(answer_keys), "seq", split_axis=0, concat_axis=2, tiled=True),
        lax.all_to_all(
            choice_entries(answer_values), "seq", split_axis=0, concat_axis=2, tiled=True
        ),
        lax.all_to_all(
            prefix_items(cached_prefix_keys), "seq", split_axis=0, concat_axis=2, tiled=True
        ),
        lax.all_to_all(
            prefix_items(cached_prefix_values), "seq", split_axis=0, concat_axis=2, tiled=True
        ),
    )
    scaling = HEAD_SIZE ** (-0.5)
    query_vector = head_queries[0].reshape(per_group, full_len, per_dev, HEAD_SIZE)
    prefix_scores = (
        jnp.einsum(
            "clhd,pd->chlp", query_vector, head_pkeys[0, 0], preferred_element_type=jnp.float32
        )
        * scaling
    )
    choice_scores = (
        jnp.einsum("clhd,csd->chls", query_vector, head_keys[0], preferred_element_type=jnp.float32)
        * scaling
    )
    causal = lax.broadcasted_iota(jnp.int32, (full_len, full_len), 0) >= lax.broadcasted_iota(
        jnp.int32, (full_len, full_len), 1
    )
    choice_scores = jnp.where(causal, choice_scores, -1e30)
    row_peak = jnp.maximum(prefix_scores.max(-1), choice_scores.max(-1))[..., None]
    prefix_exp = jnp.exp(prefix_scores - row_peak)
    choice_exp = jnp.exp(choice_scores - row_peak)
    normalizer = prefix_exp.sum(-1, keepdims=True) + choice_exp.sum(-1, keepdims=True)
    attended_output_rows = jnp.einsum(
        "chlp,pd->clhd",
        (prefix_exp / normalizer).astype(jnp.bfloat16),
        head_pvalues[0, 0],
        preferred_element_type=jnp.float32,
    )
    attended_output_rows = attended_output_rows + jnp.einsum(
        "chls,csd->clhd",
        (choice_exp / normalizer).astype(jnp.bfloat16),
        head_values[0],
        preferred_element_type=jnp.float32,
    )
    attended_output_rows = attended_output_rows.astype(jnp.bfloat16).reshape(
        per_group, full_len, per_dev * HEAD_SIZE
    )
    result_output_rows = out_weight
    if groups > 1:
        peer_device = partner(result_output_rows, "seq", 0)
        is_lower = myself % 2 == 0
        result_output_rows = jnp.where(
            is_lower,
            jnp.concatenate([result_output_rows, peer_device], 0),
            jnp.concatenate([peer_device, result_output_rows], 0),
        )
    partial_rows = jnp.einsum(
        "omp,pu->omu", attended_output_rows, result_output_rows, preferred_element_type=jnp.float32
    )
    received = lax.all_to_all(partial_rows[None], "seq", split_axis=2, concat_axis=0, tiled=True)
    summed = (
        received.reshape(grouped_heads, groups, per_group, local_length, D)
        .sum(0)
        .reshape(CHOICE_COUNT, local_length, D)
    )
    hidden = residual.astype(jnp.float32) + summed
    inv_rms = lax.rsqrt(jnp.mean(hidden * hidden, -1, keepdims=True) + 1e-05)
    normalized_hidden = (hidden * inv_rms * norm_gain).astype(jnp.bfloat16)
    logits = jnp.einsum(
        "cld,dv->clv",
        lax.all_gather(normalized_hidden, "seq", axis=1, tiled=True),
        head_weight,
        preferred_element_type=jnp.float32,
    )
    vocab_local = head_weight.shape[1]
    offsets = targets - myself * vocab_local
    vocab_col = lax.broadcasted_iota(jnp.int32, logits.shape, 2)
    target_logit = jnp.sum(jnp.where(vocab_col == offsets[..., None], logits, 0.0), -1)
    local_max = logits.max(-1)

    def fold_stats(earlier, later):
        prefix_peak_score, sum_early, hit_early = earlier
        max_late, sum_late, hit_late = later
        joined = jnp.maximum(prefix_peak_score, max_late)
        return (
            joined,
            sum_early * jnp.exp(prefix_peak_score - joined) + sum_late * jnp.exp(max_late - joined),
            hit_early + hit_late,
        )

    global_max, exp_total, target_sum = combined_all(
        (local_max, jnp.sum(jnp.exp(logits - local_max[..., None]), -1), target_logit),
        "seq",
        fold_stats,
    )
    logprobs = target_sum - global_max - jnp.log(exp_total)
    positions = lax.broadcasted_iota(jnp.int32, (CHOICE_COUNT, full_len), 1)
    usable = jnp.where((score_mask == 1) & (positions < lengths[:, None]), 1.0, 0.0)
    counted = jnp.maximum(jnp.sum(usable, -1), 1.0)
    scores = jnp.sum(logprobs * usable, -1) / counted
    return (lax.dynamic_slice_in_dim(logprobs, myself * local_length, local_length, 1), scores)

MESH = pl.DeviceIdType.MESH
SLOTS = 13
F32, BF16 = jnp.float32, jnp.bfloat16


def across(column):
    rows = column.shape[0]
    wide = jnp.broadcast_to(column, (rows, 128))
    if rows < 128:
        wide = jnp.concatenate([wide, jnp.zeros((128 - rows, 128), F32)], 0)
    return wide.T[:8]


def down(lanes, rows):
    return jnp.broadcast_to(lanes[:1], (128, 128)).T[:rows, :1]


def fused_kernel(
    n,
    queries_ref,
    residual_ref,
    ak_ref,
    av_ref,
    pk_ref,
    pv_ref,
    gain_ref,
    tgt_ref,
    mask_ref,
    lengths_ref,
    ow_ref,
    hw_ref,
    out_ref,
    wbuf,
    q_ref,
    res_ref,
    akv_ref,
    kbuf,
    vbuf,
    abuf,
    qbuf,
    rbuf,
    rows32,
    att,
    psend,
    precv,
    ysend,
    yrecv,
    sbuf,
    rsbuf,
    ssq,
    xbuf,
    acc,
    stat,
    w_sem,
    ow_sem,
    k_sem,
    v_sem,
    a_sem,
    kf_sem,
    vf_sem,
    af_sem,
    q_sem,
    r_sem,
    p_sem,
    y_sem,
    rs_sem,
    ssq_sem,
    x_sem,
    xf_sem,
    st_sem,
):
    half = n // 2
    me = lax.axis_index("seq")
    chip, par = lax.div(me, 2), lax.rem(me, 2)
    other = chip * 2 + (1 - par)
    width = ow_ref.shape[1] // n
    depth = hw_ref.shape[0] // n
    vocab = hw_ref.shape[1]
    per_msg = q_ref.shape[1]
    sub = width // 128
    rows = n * per_msg // sub
    per_slot = vocab // width
    choices = per_msg // sub
    line = half // 2
    place, side = lax.div(chip, 2), lax.rem(chip, 2)
    beside = 2 * (2 * place + 1 - side) + par

    def dev(k, parity):
        return 2 * k + parity

    def ahead(d):
        return lax.rem(chip + d, half)

    def behind(d):
        return lax.rem(chip + half - d, half)

    def remote(src, dst, sems, i, target):
        return pltpu.make_async_remote_copy(
            src_ref=src,
            dst_ref=dst,
            send_sem=sems.at[0, i],
            recv_sem=sems.at[1, i],
            device_id={"seq": target},
            device_id_type=MESH,
        )

    def toward(e):
        z = lax.rem(place + lax.div(e, 2), line)
        return 2 * z + lax.rem(side + lax.rem(e, 2), 2)

    def arrived_from(e):
        z = lax.rem(place + line - lax.div(e, 2), line)
        return 2 * z + lax.rem(side + lax.rem(e, 2), 2)

    def turn(i):
        return jnp.where(i < 2, i, jnp.where(i <= line, 2 * (i - 1), 2 * (i - line) + 1))

    def source(t):
        return dev(arrived_from(turn(lax.div(t, 2))), lax.rem(par + lax.rem(t, 2), 2))

    def head_copy(t):
        first = pl.multiple_of(source(t) * depth, depth)
        return pltpu.make_async_copy(
            hw_ref.at[pl.ds(first, depth), :], wbuf.at[lax.rem(t, SLOTS)], w_sem.at[t]
        )

    def proj_copy(i):
        return pltpu.make_async_copy(
            ow_ref.at[:, pl.ds(pl.multiple_of(i * vocab, vocab), vocab)],
            wbuf.at[SLOTS - 2 + i],
            ow_sem.at[i],
        )

    proj_copy(0).start()
    proj_copy(1).start()

    @pl.loop(0, SLOTS - 2)
    def _(t):
        head_copy(t).start()

    barrier = pltpu.get_barrier_semaphore()

    @pl.loop(1, n)
    def _(d):
        pl.semaphore_signal(
            barrier, inc=1, device_id={"seq": lax.rem(me + d, n)}, device_id_type=MESH
        )

    def staged(ref, msg):
        @pl.loop(0, n)
        def _(j):
            for c in range(choices):
                for h in range(sub):
                    lanes = pl.ds(pl.multiple_of(j * width + h * 128, 128), 128)
                    row = pl.ds(j * per_msg + c * sub + h, 1)
                    rows32[row, :] = ref[:, lanes].astype(F32)[c : c + 1]

        msg[...] = rows32[...].reshape(n, per_msg, 128).astype(BF16)

    rows32[...] = jnp.zeros_like(rows32)

    @pl.loop(0, half)
    def _(k):
        lanes = pl.ds(pl.multiple_of(k * 128, 128), 128)
        for c in range(choices):
            rows32[pl.ds(k * 32 + c, 1), :] = ak_ref[:, lanes].astype(F32)[c : c + 1]
            rows32[pl.ds(k * 32 + 16 + c, 1), :] = av_ref[:, lanes].astype(F32)[c : c + 1]

    akv_ref[...] = rows32[...].reshape(half, 32, 128).astype(BF16)
    staged(queries_ref, q_ref)
    staged(residual_ref, res_ref)

    pl.semaphore_wait(barrier, n - 1)

    def kv_sends(d):
        k = ahead(d)
        cols = pl.ds(pl.multiple_of(k * 128, 128), 128)
        to = dev(k, par)
        return (
            remote(pk_ref.at[:, cols], kbuf.at[me], k_sem, d, to),
            remote(pv_ref.at[:, cols], vbuf.at[me], v_sem, d, to),
            remote(akv_ref.at[k], abuf.at[me], a_sem, d, to),
        )

    def kv_forwards(d):
        s = dev(behind(d), par)
        return (
            remote(kbuf.at[s], kbuf.at[s], kf_sem, d, other),
            remote(vbuf.at[s], vbuf.at[s], vf_sem, d, other),
            remote(abuf.at[s], abuf.at[s], af_sem, d, other),
        )

    def kv_arrivals(d):
        s = dev(behind(d), par)
        return (
            remote(kbuf.at[s], kbuf.at[s], k_sem, d, other),
            remote(vbuf.at[s], vbuf.at[s], v_sem, d, other),
            remote(abuf.at[s], abuf.at[s], a_sem, d, other),
        )

    def kv_relayed(d):
        s = dev(behind(d), 1 - par)
        return (
            remote(kbuf.at[s], kbuf.at[s], kf_sem, d, other),
            remote(vbuf.at[s], vbuf.at[s], vf_sem, d, other),
            remote(abuf.at[s], abuf.at[s], af_sem, d, other),
        )

    def kv_own():
        cols = pl.ds(pl.multiple_of(chip * 128, 128), 128)
        return (
            remote(pk_ref.at[:, cols], kbuf.at[me], kf_sem, 0, other),
            remote(pv_ref.at[:, cols], vbuf.at[me], vf_sem, 0, other),
            remote(akv_ref.at[chip], abuf.at[me], af_sem, 0, other),
        )

    def q_send(d):
        to = lax.rem(me + d, n)
        return remote(q_ref.at[to], qbuf.at[me], q_sem, d, to)

    def q_arrival(d):
        s = lax.rem(me + n - d, n)
        return remote(qbuf.at[s], qbuf.at[s], q_sem, d, other)

    def r_send(d):
        to = lax.rem(me + d, n)
        return remote(res_ref.at[to], rbuf.at[me], r_sem, d, to)

    def r_arrival(d):
        s = lax.rem(me + n - d, n)
        return remote(rbuf.at[s], rbuf.at[s], r_sem, d, other)

    @pl.loop(1, half)
    def _(d):
        for copy in kv_sends(d):
            copy.start()

    for copy in kv_own():
        copy.start()

    @pl.loop(1, n)
    def _(d):
        q_send(d).start()

    @pl.loop(1, n)
    def _(d):
        r_send(d).start()

    own_cols = pl.ds(pl.multiple_of(chip * 128, 128), 128)
    kbuf[me] = pk_ref[:, own_cols]
    vbuf[me] = pv_ref[:, own_cols]
    abuf[me] = akv_ref[chip]
    qbuf[me] = q_ref[me]
    rbuf[me] = res_ref[me]

    @pl.loop(1, half)
    def _(d):
        for arrived, onward in zip(kv_arrivals(d), kv_forwards(d)):
            arrived.wait_recv()
            onward.start()

    @pl.loop(1, n)
    def _(d):
        q_arrival(d).wait_recv()

    @pl.loop(0, half)
    def _(d):
        for copy in kv_relayed(d):
            copy.wait_recv()

    count = n * per_msg
    keys = kbuf[...].reshape(-1, 128)
    values = vbuf[...].reshape(-1, 128)
    own_keys = abuf[:, :16].reshape(-1, 128)
    own_values = abuf[:, 16:].reshape(-1, 128)
    scaling = HEAD_SIZE ** (-0.5)
    block = 64
    nt = (((1,), (1,)), ((), ()))

    @pl.loop(0, count // block)
    def _(i):
        per = block // per_msg
        qs = qbuf[pl.ds(i * per, per)].reshape(block, 128)
        ps = lax.dot_general(qs, keys, nt, preferred_element_type=F32) * scaling
        cs = lax.dot_general(qs, own_keys, nt, preferred_element_type=F32) * scaling
        row = lax.broadcasted_iota(jnp.int32, cs.shape, 0) + i * block
        col = lax.broadcasted_iota(jnp.int32, cs.shape, 1)
        choice = (row % per_msg) // sub
        seen = (choice == col % 16) & (col // 16 <= row // per_msg)
        cs = jnp.where(seen, cs, -1e30)
        top = jnp.maximum(ps.max(-1, keepdims=True), cs.max(-1, keepdims=True))
        pe, ce = jnp.exp(ps - top), jnp.exp(cs - top)
        inverse = 1.0 / (pe.sum(-1, keepdims=True) + ce.sum(-1, keepdims=True))
        mixed = jnp.dot((pe * inverse).astype(BF16), values, preferred_element_type=F32)
        mixed += jnp.dot((ce * inverse).astype(BF16), own_values, preferred_element_type=F32)
        rows32[pl.ds(pl.multiple_of(i * block, block), block), :] = mixed

    def regroup():
        return jnp.concatenate(
            [
                jnp.concatenate(
                    [rows32[pl.ds(c * sub + h, n, stride=per_msg), :] for h in range(sub)],
                    axis=1,
                )
                for c in range(choices)
            ],
            axis=0,
        )

    att[...] = regroup().astype(BF16)

    proj_copy(0).wait()
    proj_copy(1).wait()

    def projected(j):
        slot = SLOTS - 2 + lax.div(j, per_slot)
        cols = pl.ds(pl.multiple_of(lax.rem(j, per_slot) * width, width), width)
        return jnp.dot(att[...], wbuf[slot, :, cols], preferred_element_type=F32)

    def p_send(d):
        return remote(psend.at[d], precv.at[d], p_sem, d, other)

    def y_send(d):
        return remote(ysend.at[d], yrecv.at[d], y_sem, d, beside)

    def rs_send(d):
        return remote(sbuf.at[d], rsbuf.at[d], rs_sem, d, dev(toward(2 * d), par))

    def give(e):
        psend[e] = projected(dev(toward(e), 1 - par))
        p_send(e).start()

    def chip_sum(e):
        mine = projected(dev(toward(e), par))
        p_send(e).wait_recv()
        return mine + precv[e]

    @pl.loop(1, line + 1)
    def _(d):
        give(2 * lax.rem(d, line) + 1)

    @pl.loop(1, line + 1)
    def _(d):
        give(2 * lax.rem(d, line))

    @pl.loop(1, line + 1)
    def _(i):
        d = lax.rem(i, line)
        ysend[d] = chip_sum(2 * d + 1).astype(BF16)
        y_send(d).start()

    @pl.loop(1, line)
    def _(d):
        mine = chip_sum(2 * d)
        y_send(d).wait_recv()
        sbuf[d] = (mine + yrecv[d].astype(F32)).astype(BF16)
        rs_send(d).start()

    mine = chip_sum(0)

    @pl.loop(SLOTS - 2, SLOTS)
    def _(t):
        head_copy(t).start()

    @pl.loop(1, n)
    def _(d):
        r_arrival(d).wait_recv()

    rows32[...] = rbuf[...].astype(F32).reshape(count, 128)
    y_send(0).wait_recv()
    total = regroup() + (mine + yrecv[0].astype(F32))
    for d in range(1, line):
        rs_send(d).wait_recv()
        total = total + rsbuf[d].astype(F32)

    def ssq_send(d):
        return remote(ssq.at[me], ssq.at[me], ssq_sem, d, lax.rem(me + d, n))

    def ssq_arrival(d):
        s = lax.rem(me + n - d, n)
        return remote(ssq.at[s], ssq.at[s], ssq_sem, d, other)

    ssq[me] = across(jnp.sum(total * total, -1, keepdims=True))

    @pl.loop(1, n)
    def _(d):
        ssq_send(d).start()

    @pl.loop(1, n)
    def _(d):
        ssq_arrival(d).wait_recv()

    squares = down(jnp.sum(ssq[...], 0), rows)
    inv_rms = lax.rsqrt(squares / (n * width) + 1e-05)
    gain = gain_ref[:, pl.ds(pl.multiple_of(me * width, width), width)]
    xbuf[me] = (total * inv_rms * gain).astype(BF16)

    def x_send(d):
        return remote(xbuf.at[me], xbuf.at[me], x_sem, 2 * d, dev(toward(2 * d), par))

    def x_aside(e):
        s = dev(arrived_from(e), par)
        return remote(xbuf.at[s], xbuf.at[s], x_sem, e + 1, beside)

    def x_arrival(e):
        s = dev(arrived_from(e), par)
        return remote(xbuf.at[s], xbuf.at[s], x_sem, e, other)

    def x_forward(e):
        s = dev(arrived_from(e), par)
        return remote(xbuf.at[s], xbuf.at[s], xf_sem, e, other)

    def x_relayed(e):
        s = dev(arrived_from(e), 1 - par)
        return remote(xbuf.at[s], xbuf.at[s], xf_sem, e, other)

    x_aside(0).start()

    @pl.loop(1, line)
    def _(d):
        x_send(d).start()

    x_forward(0).start()
    acc[...] = jnp.zeros_like(acc)
    tile = 1024 if vocab % 1024 == 0 else vocab

    def step(t):
        head_copy(t).wait()
        slot = lax.rem(t, SLOTS)
        x = xbuf[source(t)]
        for first in range(0, vocab, tile):
            acc[:, first : first + tile] += jnp.dot(
                x, wbuf[slot, :, first : first + tile], preferred_element_type=F32
            )

        @pl.when(t + SLOTS < n)
        def _():
            head_copy(t + SLOTS).start()

    @pl.loop(0, half)
    def _(i):
        e = turn(i)

        @pl.when(i > 0)
        def _():
            x_arrival(e).wait_recv()

            @pl.when(lax.rem(e, 2) == 0)
            def _():
                x_aside(e).start()

            x_forward(e).start()

        step(2 * i)
        x_relayed(e).wait_recv()
        step(2 * i + 1)

    logits = acc[...]
    peak = logits.max(-1, keepdims=True)
    total_exp = jnp.sum(jnp.exp(logits - peak), -1, keepdims=True)
    ids = tgt_ref[...].astype(F32)
    row = lax.broadcasted_iota(jnp.int32, (rows, n), 0)
    slot = lax.broadcasted_iota(jnp.int32, (rows, n), 1)
    wanted = jnp.zeros((rows, n), F32)
    for c in range(choices):
        mine_here = (row // n == c) & (row % n == slot)
        wanted = jnp.where(mine_here, ids[c : c + 1], wanted)
    wanted = jnp.sum(wanted, -1, keepdims=True).astype(jnp.int32)
    vocab_col = lax.broadcasted_iota(jnp.int32, logits.shape, 1) + me * vocab
    hit = jnp.sum(jnp.where(vocab_col == wanted, logits, 0.0), -1, keepdims=True)
    lane = lax.broadcasted_iota(jnp.int32, (8, 128), 0)
    stat[me] = jnp.where(
        lane == 0, across(peak), jnp.where(lane == 1, across(total_exp), across(hit))
    )

    def st_send(d):
        return remote(stat.at[me], stat.at[me], st_sem, d, lax.rem(me + d, n))

    def st_arrival(d):
        s = lax.rem(me + n - d, n)
        return remote(stat.at[s], stat.at[s], st_sem, d, other)

    @pl.loop(1, n)
    def _(d):
        st_send(d).start()

    @pl.loop(1, n)
    def _(d):
        st_arrival(d).wait_recv()

    everything = stat[...]
    peaks, sums, hits = everything[:, 0:1], everything[:, 1:2], everything[:, 2:3]
    top = jnp.max(peaks, 0)
    whole = jnp.sum(sums * jnp.exp(peaks - top[None]), 0)
    logprob = jnp.sum(hits, 0) - top - jnp.log(whole)
    table = jnp.concatenate([logprob[:, c * n : (c + 1) * n] for c in range(choices)], 0)
    position = lax.broadcasted_iota(jnp.int32, table.shape, 1)
    choice = lax.broadcasted_iota(jnp.int32, table.shape, 0)
    own = jnp.sum(jnp.where(position == me, table, 0.0), -1, keepdims=True)
    length = jnp.zeros(table.shape, jnp.int32)
    for c in range(choices):
        length = jnp.where(choice == c, lengths_ref[c], length)
    usable = jnp.where((mask_ref[...] == 1) & (position < length), 1.0, 0.0)
    counted = jnp.maximum(jnp.sum(usable, -1, keepdims=True), 1.0)
    means = jnp.sum(table * usable, -1, keepdims=True) / counted
    diagonal = lax.broadcasted_iota(jnp.int32, (choices, 128), 0) == lax.broadcasted_iota(
        jnp.int32, (choices, 128), 1
    )

    def flat(column):
        wide = jnp.broadcast_to(column, (choices, 128))
        return jnp.sum(jnp.where(diagonal, wide, 0.0), 0, keepdims=True)

    first = lax.broadcasted_iota(jnp.int32, (8, 128), 0) == 0
    out_ref[...] = jnp.where(first, flat(own), flat(means))

    @pl.loop(1, half)
    def _(d):
        for copy in kv_sends(d) + kv_forwards(d):
            copy.wait_send()

    @pl.loop(1, line)
    def _(d):
        rs_send(d).wait_send()
        x_send(d).wait_send()

    @pl.loop(0, line)
    def _(d):
        y_send(d).wait_send()
        x_aside(2 * d).wait_send()

    for copy in kv_own():
        copy.wait_send()

    @pl.loop(0, half)
    def _(d):
        p_send(d).wait_send()
        x_forward(d).wait_send()

    @pl.loop(1, n)
    def _(d):
        q_send(d).wait_send()
        r_send(d).wait_send()
        ssq_send(d).wait_send()
        st_send(d).wait_send()


def fused(
    queries,
    answer_keys,
    answer_values,
    cached_prefix_keys,
    cached_prefix_values,
    residual,
    out_weight,
    norm_gain,
    head_weight,
    targets,
    score_mask,
    lengths,
):
    n = lax.axis_size("seq")
    half = n // 2
    width = D // n
    sub = width // HEAD_SIZE
    per_msg = CHOICE_COUNT * sub
    rows = CHOICE_COUNT * n
    local_prefix = cached_prefix_keys.shape[0]
    vocab = head_weight.shape[1]
    vmem, hbm = (
        pl.BlockSpec(memory_space=pltpu.VMEM),
        pl.BlockSpec(memory_space=pl.ANY),
    )
    sems = pltpu.SemaphoreType.DMA
    smem = pl.BlockSpec(memory_space=pltpu.SMEM)
    message = pltpu.VMEM((n, per_msg, HEAD_SIZE), BF16)
    packed = pl.pallas_call(
        functools.partial(fused_kernel, n),
        out_shape=jax.ShapeDtypeStruct((8, 128), F32),
        in_specs=[vmem] * 9 + [smem] + [hbm] * 2,
        out_specs=vmem,
        scratch_shapes=[
            pltpu.VMEM((SLOTS, width, vocab), BF16),
            message,
            message,
            pltpu.VMEM((half, 32, HEAD_SIZE), BF16),
            pltpu.VMEM((n, local_prefix, HEAD_SIZE), BF16),
            pltpu.VMEM((n, local_prefix, HEAD_SIZE), BF16),
            pltpu.VMEM((n, 32, HEAD_SIZE), BF16),
            pltpu.VMEM((n, per_msg, HEAD_SIZE), BF16),
            pltpu.VMEM((n, per_msg, HEAD_SIZE), BF16),
            pltpu.VMEM((n * per_msg, HEAD_SIZE), F32),
            pltpu.VMEM((rows, width), BF16),
            pltpu.VMEM((half, rows, width), F32),
            pltpu.VMEM((half, rows, width), F32),
            pltpu.VMEM((half // 2, rows, width), BF16),
            pltpu.VMEM((half // 2, rows, width), BF16),
            pltpu.VMEM((half // 2, rows, width), BF16),
            pltpu.VMEM((half // 2, rows, width), BF16),
            pltpu.VMEM((n, 8, 128), F32),
            pltpu.VMEM((n, rows, width), BF16),
            pltpu.VMEM((rows, vocab), F32),
            pltpu.VMEM((n, 8, 128), F32),
            sems((n,)),
            sems((2,)),
        ]
        + [sems((2, half))] * 6
        + [sems((2, n))] * 2
        + [sems((2, half))]
        + [sems((2, half // 2))] * 2
        + [sems((2, n))]
        + [sems((2, half))] * 2
        + [sems((2, n))],
        compiler_params=pltpu.CompilerParams(
            collective_id=0, has_side_effects=True, vmem_limit_bytes=67043328
        ),
    )(
        *(part.transpose(1, 0, 2)[0] for part in (queries, residual, answer_keys, answer_values)),
        cached_prefix_keys,
        cached_prefix_values,
        norm_gain.reshape(1, D),
        targets,
        score_mask,
        lengths,
        out_weight,
        head_weight,
    )
    return packed[:1, :CHOICE_COUNT].T, packed[1, :CHOICE_COUNT]


def either(*arrays):
    queries, head_weight = arrays[0], arrays[8]
    n = lax.axis_size("seq")
    small = n == 2 * KEY_VALUE_HEADS and queries.shape[1] == 1
    if small and head_weight.shape[1] * 2 == D:
        return fused(*arrays)
    return per_device(*arrays)


def solution(mesh):
    placed = (
        P("grp", "seq", None),
        P("grp", "seq", None),
        P("grp", "seq", None),
        P(("grp", "seq"), None),
        P(("grp", "seq"), None),
        P("grp", "seq", None),
        P("seq", None),
        P(),
        P(None, "seq"),
        P("grp", None),
        P("grp", None),
        P("grp"),
    )
    return jax.shard_map(
        either,
        mesh=mesh,
        in_specs=placed,
        out_specs=(P("grp", "seq"), P("grp")),
        check_vma=False,
    )
```
